32 devices in a mesh: tile: 8 (over z, x), conv: 4 (over y, core).
Axes of the slice: x: 2, y: 2, z: 4, core: 2. Of those that a mesh axis runs over, the one named last changes fastest.
Arguments:
- field: float32 [256, 24576], P(None, ('tile', 'conv')), may hold values from -6 to 6
- interp: bfloat16 [32768, 384], P(('tile', 'conv')), may hold values from -0.1875 to 0.1875
- conv_blocks: bfloat16 [64, 3, 256, 256], P(('tile', 'conv')), may hold values from -0.21875 to 0.21875
- band_shift: int32 [64, 3], P(('tile', 'conv')), may hold values from 0 to 1
- owner: int32 [12288, 1], P(('tile', 'conv')), may hold values from 0 to 3; in each aligned block of 384 rows (0 to 383, 384 to 767, ...) at most 128 rows name the same one
- edge_index: int32 [64, 128], P(('tile', 'conv')), may hold values from 0 to 767, as said below
Outputs:
- correlated: float32 [256, 24576], P(None, ('tile', 'conv'))
The draws below stay inside these ranges and needn't reach their ends.
Inputs may be any that keep to these rules, and one draw needn't show every extreme that they name: `edge_index`: row 2b lists the first 128 columns of domain b in some order, row 2b + 1 its last 128 columns in some order. Among the 384 points of one domain no owner is named more than 128 times, and in some domains one owner is named exactly 128 times.
All inputs are finite; a program needn't handle non-finite values.
Results may differ from the reference program's by a relative error of at most 0.0049.
Values may be sent and summed in bfloat16 or wider, within the bound.
No kernel may reach another device: no remote copies, remote signals or barrier semaphores. Data moves between devices by JAX's collectives and lax.ppermute only.
A program may use at most 64 MiB of HBM per device.

```python
import math
import jax
import jax.numpy as jnp
import numpy as np
from jax import lax

COLUMNS = 768
HALO_WIDTH = 128
BLOCK_POINTS = 256
OWNER_BLOCKS = 2
BAND_COUNT = 3
FIELD_ROWS = 256
DOMAINS = 32
ALL_COLUMNS = 24576
EXTENDED = 1024
SLOTS = 512
SUBPOINTS = 384
CAPACITY = 128
ALL_SUBPOINTS = 12288
N_TILE = 8
N_CONV = 4


def draw_edge_index(key, part):
    row_keys = jax.random.split(key, 2 * DOMAINS)
    orders = jax.vmap(lambda single: jax.random.permutation(single, HALO_WIDTH))(row_keys)
    side_flags = jnp.arange(2 * DOMAINS, dtype=jnp.int32) % 2
    offsets = side_flags * (COLUMNS - HALO_WIDTH)
    return (orders.astype(jnp.int32) + offsets[:, None]).astype(jnp.int32)


def with_ends(values, own_key, smallest, high):
    longest = values.shape.index(max(values.shape))
    spots = []
    for shift in (0, 1):
        where = [jax.random.randint(jax.random.fold_in(own_key, axis), (), 0, length) for axis, length in enumerate(values.shape)]
        where[longest] = (where[longest] + shift) % values.shape[longest]
        spots.append(tuple(where))
    return values.at[spots[0]].set(smallest).at[spots[1]].set(high)


def steps_of(key, shape, cuts, low, top_value):
    gain, own = 1.0, jax.random.fold_in(key, 6)
    for axis_at, shards_of in cuts:
        steps = jnp.exp(jax.random.uniform(jax.random.fold_in(own, axis_at), (shards_of,), jnp.float32, low / len(cuts), top_value / len(cuts)))
        gain = gain * jnp.repeat(steps, shape[axis_at] // shards_of).reshape([-1 if axis == axis_at else 1 for axis in range(len(shape))])
    return gain


def routed_block(own_key, own, number, rows, amount, top, limit, skew):
    sequence = jax.random.permutation(own_key, amount)
    crowded, ordinary = portions_of(amount, rows * top, limit, skew, True), portions_of(amount, rows * top, limit, skew, False)
    places = jnp.arange(amount)

    def named(sizes, rotation):
        used = int((sizes > 0).sum())
        fixed = max(1, used // 4)
        passed = fixed + (places - fixed + rotation * (used - fixed)) % max(1, amount - fixed)
        return jnp.zeros((amount,), jnp.int32).at[sequence[jnp.where(places < fixed, places, passed)]].set(jnp.asarray(sizes, jnp.int32))

    sizes = jnp.where(number % 4 == 0, named(crowded, number // 4), named(ordinary, number - number // 4 - 1))
    mixed = jax.random.permutation(jax.random.fold_in(own, 3), amount)
    source_of, taker = mixed[0:amount // 2 * 2:2], mixed[1:amount // 2 * 2:2]
    room = jnp.minimum(sizes[source_of] - 1, limit - sizes[taker]) // 2
    room = jnp.where((source_of == sequence[0]) | (taker == sequence[0]) | (sizes[taker] == 0), 0, jnp.maximum(room, 0))
    passed = jax.random.randint(jax.random.fold_in(own, 4), (amount // 2,), 0, 1 << 20) % (room + 1)
    sizes = sizes.at[source_of].add(-passed).at[taker].add(passed)
    members = jnp.searchsorted(jnp.cumsum(sizes), jnp.arange(rows * top), side="right").astype(jnp.int32)
    listing = members.reshape(top, rows).T
    listing = listing[jax.random.permutation(jax.random.fold_in(own, 1), rows)]
    rotation = jax.random.randint(jax.random.fold_in(own, 2), (rows, 1), 0, top)
    return jnp.take_along_axis(listing, (jnp.arange(top)[None, :] + rotation) % top, axis=1)


def portions_of(count, total, reach, slope, full):
    loads = [(1 << 20) // math.isqrt(grade ** slope) + 1 for grade in range(1, count + 1)]
    largest = reach if full else min(reach, max(-(-total // count), total * loads[0] // sum(loads)))
    least = 1 if total - largest >= count - 1 else 0
    holding, surplus = [largest] + [least] * (count - 1), total - largest - least * (count - 1)
    while surplus > 0:
        movable = [i for i in range(1, count) if holding[i] < largest] or [i for i in range(1, count) if holding[i] < reach]
        mass, remaining = sum([loads[i] for i in movable]), surplus
        for i in movable:
            addition = min(reach - holding[i], max(1, remaining * loads[i] // mass), surplus)
            holding[i] = holding[i] + addition
            surplus = surplus - addition
    return np.array(holding)


def gaussian(stream_key, dims, width, limit, cuts=(), kind=jnp.bfloat16):
    drawn = width * jax.random.normal(stream_key, dims, jnp.float32)
    if cuts:
        drawn = drawn * steps_of(stream_key, dims, cuts, -0.22, 0.18)
    return jnp.clip(drawn, -limit, limit).astype(kind)


def setup_inputs(seed: int = 0) -> dict:
    streams_of = jax.random.split(jax.random.key(seed), 7)
    field = gaussian(streams_of[0], (FIELD_ROWS, ALL_COLUMNS), 1.0, 6.0, ((1, 32),), jnp.float32)
    interp = gaussian(streams_of[1], (DOMAINS * EXTENDED, SUBPOINTS), EXTENDED ** -0.5, 0.1875, ((0, 32),))
    conv_blocks = gaussian(streams_of[2], (DOMAINS * OWNER_BLOCKS, BAND_COUNT, BLOCK_POINTS, BLOCK_POINTS), (BAND_COUNT * BLOCK_POINTS) ** -0.5, 0.21875, ((0, 32),))
    band_shift = with_ends(jax.random.randint(streams_of[3], (DOMAINS * OWNER_BLOCKS, BAND_COUNT), 0, OWNER_BLOCKS), jax.random.fold_in(streams_of[3], 1), 0, OWNER_BLOCKS - 1).astype(jnp.int32)
    owner_keys = jax.random.split(jax.random.fold_in(streams_of[4], 1), ALL_SUBPOINTS // SUBPOINTS)
    owner_turns = jax.random.permutation(jax.random.fold_in(streams_of[4], 3), ALL_SUBPOINTS // SUBPOINTS)
    owner = jax.vmap(lambda own, number: routed_block(jax.random.fold_in(streams_of[4], 2), own, number, SUBPOINTS, N_CONV, 1, CAPACITY, 2))(owner_keys, owner_turns).reshape((ALL_SUBPOINTS, 1))
    edge_index = draw_edge_index(jax.random.fold_in(streams_of[6], 71), 0)
    return dict(field=field, interp=interp, conv_blocks=conv_blocks, band_shift=band_shift, owner=owner, edge_index=edge_index)


def slot_table(owners):
    choose = (owners[:, None] == jnp.arange(N_CONV, dtype=jnp.int32)[None, :]).astype(jnp.int32)
    before = jnp.cumsum(choose, axis=0) - choose
    position = jnp.sum(before * choose, axis=1)
    slot_index = owners * CAPACITY + position
    return (slot_index[:, None] == jnp.arange(SLOTS, dtype=jnp.int32)[None, :]).astype(jnp.float32)


def interpolate(operands):
    extended, weights, owners = operands
    subgrid = jnp.dot(extended, weights, preferred_element_type=jnp.float32).astype(jnp.bfloat16)
    packed = jnp.dot(subgrid.astype(jnp.float32), slot_table(owners), precision=lax.Precision.HIGHEST)
    return packed.astype(jnp.bfloat16)


def convolve(operands):
    values, blocks, shifts = operands
    height = values.shape[0]
    pieces = values.reshape(height, OWNER_BLOCKS, BLOCK_POINTS).astype(jnp.float32)
    source = (jnp.arange(OWNER_BLOCKS, dtype=jnp.int32)[:, None] + shifts) % OWNER_BLOCKS
    picked = pieces[:, source, :]
    matrices = blocks.astype(jnp.float32)
    forward = jnp.einsum("rjbp,jbpq->rjq", picked, matrices, precision=lax.Precision.HIGHEST).astype(jnp.bfloat16)
    backward = jnp.einsum("rjq,jbpq->rjbp", forward.astype(jnp.float32), matrices, precision=lax.Precision.HIGHEST)
    select = (source[:, :, None] == jnp.arange(OWNER_BLOCKS, dtype=jnp.int32)[None, None, :]).astype(jnp.float32)
    adjoint = jnp.einsum("rjbp,jbs->rsp", backward, select, precision=lax.Precision.HIGHEST)
    return adjoint.reshape(height, SLOTS).astype(jnp.bfloat16)


def adjoint_interpolate(operands):
    returned_slots, weights, owners = operands
    returned = jnp.dot(returned_slots.astype(jnp.float32), slot_table(owners).T, precision=lax.Precision.HIGHEST)
    returned = returned.astype(jnp.bfloat16)
    return jnp.dot(returned, weights.T, preferred_element_type=jnp.float32)


def add_edges(inner_part, left_sum, right_sum, left_list, right_list):
    inner_part = inner_part.at[:, left_list].add(left_sum)
    return inner_part.at[:, right_list].add(right_sum)


def reference(field, interp, conv_blocks, band_shift, owner, edge_index):
    field_rows = field.shape[0]
    rounded = field.astype(jnp.bfloat16).reshape(field_rows, DOMAINS, COLUMNS).transpose(1, 0, 2)
    edges = edge_index.reshape(DOMAINS, 2, HALO_WIDTH)
    left_lists = edges[:, 0, :]
    right_lists = edges[:, 1, :]
    left_index = jnp.broadcast_to(left_lists[:, None, :], (DOMAINS, field_rows, HALO_WIDTH))
    right_index = jnp.broadcast_to(right_lists[:, None, :], (DOMAINS, field_rows, HALO_WIDTH))
    left_values = jnp.take_along_axis(rounded, left_index, axis=2)
    right_values = jnp.take_along_axis(rounded, right_index, axis=2)
    extended = jnp.concatenate([jnp.roll(right_values, 1, axis=0), rounded, jnp.roll(left_values, -1, axis=0)], axis=2)
    weights = interp.reshape(DOMAINS, EXTENDED, SUBPOINTS)
    owners = owner.reshape(DOMAINS, SUBPOINTS)
    packed = lax.map(interpolate, (extended, weights, owners))
    gathered = packed.reshape(N_TILE, N_CONV, field_rows, N_CONV, CAPACITY).transpose(0, 3, 2, 1, 4)
    gathered = gathered.reshape(DOMAINS, field_rows, SLOTS)
    blocks = conv_blocks.reshape(DOMAINS, OWNER_BLOCKS, BAND_COUNT, BLOCK_POINTS, BLOCK_POINTS)
    shifts = band_shift.reshape(DOMAINS, OWNER_BLOCKS, BAND_COUNT)
    adjoints = lax.map(convolve, (gathered, blocks, shifts))
    returned = adjoints.reshape(N_TILE, N_CONV, field_rows, N_CONV, CAPACITY).transpose(0, 3, 2, 1, 4)
    returned = returned.reshape(DOMAINS, field_rows, SLOTS)
    partial_value = lax.map(adjoint_interpolate, (returned, weights, owners))
    interior = partial_value[:, :, HALO_WIDTH:HALO_WIDTH + COLUMNS]
    left_sums = jnp.roll(partial_value[:, :, HALO_WIDTH + COLUMNS:], 1, axis=0)
    right_sums = jnp.roll(partial_value[:, :, :HALO_WIDTH], -1, axis=0)
    result = jax.vmap(add_edges)(interior, left_sums, right_sums, left_lists, right_lists)
    return result.transpose(1, 0, 2).reshape(field_rows, DOMAINS * COLUMNS)
```

```python
import functools

import jax
import jax.numpy as jnp
from jax import lax
from jax.experimental import pallas as pl
from jax.experimental.pallas import tpu as pltpu
from jax.sharding import PartitionSpec as P


F32 = jnp.float32
BF16 = jnp.bfloat16
VMEM = pl.BlockSpec(memory_space=pltpu.VMEM)
SMEM = pl.BlockSpec(memory_space=pltpu.SMEM)


def dot(a, b):
    return jnp.dot(a, b, preferred_element_type=F32)


def dot_last(a, b):
    return lax.dot_general(a, b, (((1,), (1,)), ((), ())), preferred_element_type=F32)


def one_hot_columns(edge_row, offset):
    width = edge_row.shape[1]
    column = lax.broadcasted_iota(jnp.int32, (width, width), 0)
    return (column + offset == edge_row).astype(F32).astype(BF16)


def rims_kernel(columns, head_ref, tail_ref, edge_ref, left_ref, right_ref):
    width = edge_ref.shape[1]
    left = one_hot_columns(edge_ref[0:1, :], 0)
    right = one_hot_columns(edge_ref[1:2, :], columns - width)
    left_ref[...] = dot(head_ref[...].astype(BF16), left).astype(BF16)
    right_ref[...] = dot(tail_ref[...].astype(BF16), right).astype(BF16)


def interior_kernel(groups, capacity, me_ref, field_ref, interp_ref, owner_ref, mid_ref, place_ref):
    columns = field_ref.shape[1]
    rim = (interp_ref.shape[0] - columns) // 2
    points = owner_ref.shape[1]
    mid_ref[...] = dot(field_ref[...].astype(BF16), interp_ref[rim : rim + columns, :])
    owners = owner_ref[...]
    group = lax.broadcasted_iota(jnp.int32, (max(groups, 16), points), 0)
    choose = (group == owners).astype(F32)
    earlier = lax.broadcasted_iota(jnp.int32, (points, points), 0) < lax.broadcasted_iota(
        jnp.int32, (points, points), 1
    )
    before = dot(choose.astype(BF16), earlier.astype(F32).astype(BF16))
    rank = jnp.sum(before * choose, axis=0, keepdims=True).astype(jnp.int32)
    slot = jnp.bitwise_xor(owners, me_ref[0]) * capacity + rank
    slots = lax.broadcasted_iota(jnp.int32, (groups * capacity, points), 0)
    place_ref[...] = (slots == slot).astype(F32).astype(BF16)


def subgrid_kernel(groups, mid_ref, from_left_ref, from_right_ref, interp_ref, place_ref, *outs):
    rim = from_left_ref.shape[1]
    high = interp_ref.shape[0] - rim
    subgrid = mid_ref[...] + dot(from_left_ref[...], interp_ref[:rim, :])
    subgrid = (subgrid + dot(from_right_ref[...], interp_ref[high:, :])).astype(BF16)
    packed = dot_last(subgrid, place_ref[...]).astype(BF16)
    capacity = packed.shape[1] // groups
    for step in range(groups):
        outs[step][...] = packed[:, step * capacity : (step + 1) * capacity]


def convolve_kernel(groups, me_ref, shift_ref, *refs):
    inputs = refs[:groups]
    conv_ref = refs[groups]
    outs = refs[groups + 1 : 2 * groups + 1]
    bands_ref, gathered_ref, adjoint_ref = refs[2 * groups + 1 :]
    me = me_ref[0]
    blocks, bands, points = conv_ref.shape[0], conv_ref.shape[1], conv_ref.shape[2]
    capacity = inputs[0].shape[1]
    per = points // capacity
    for step in range(groups):
        bands_ref[step] = inputs[step][...]
    for domain in range(groups):
        at = (domain % per) * capacity
        gathered_ref[domain // per, :, at : at + capacity] = bands_ref[jnp.bitwise_xor(me, domain)]
    adjoint_ref[...] = jnp.zeros_like(adjoint_ref)
    for j in range(blocks):
        source = [lax.rem(j + shift_ref[j, c], blocks) for c in range(bands)]
        forward = dot(gathered_ref[source[0]], conv_ref[j, 0])
        for c in range(1, bands):
            forward = forward + dot(gathered_ref[source[c]], conv_ref[j, c])
        forward = forward.astype(BF16)
        for c in range(bands):
            adjoint_ref[source[c]] += dot_last(forward, conv_ref[j, c])
    for domain in range(groups):
        at = (domain % per) * capacity
        bands_ref[domain] = adjoint_ref[domain // per, :, at : at + capacity].astype(BF16)
    for step in range(groups):
        outs[step][...] = bands_ref[jnp.bitwise_xor(me, step)]


def edge_partial_kernel(groups, rim, *refs):
    inputs = refs[:groups]
    place_ref, interp_ref, returned_ref, left_ref, right_ref = refs[groups:]
    packed = jnp.concatenate([ref[...] for ref in inputs], axis=1)
    returned = dot(packed, place_ref[...]).astype(BF16)
    returned_ref[...] = returned
    high = interp_ref.shape[0] - rim
    left_ref[...] = dot_last(returned, interp_ref[:rim, :]).astype(BF16)
    right_ref[...] = dot_last(returned, interp_ref[high:, :]).astype(BF16)


def interior_partial_kernel(rim, returned_ref, interp_ref, out_ref):
    high = interp_ref.shape[0] - rim
    out_ref[...] = dot_last(returned_ref[...], interp_ref[rim:high, :])


def add_edges_kernel(columns, from_left_ref, from_right_ref, edge_ref, inner_ref, out_ref):
    width = edge_ref.shape[1]
    side = pl.program_id(0)

    @pl.when(side == 0)
    def _():
        left = one_hot_columns(edge_ref[0:1, :], 0)
        out_ref[...] = inner_ref[...] + dot_last(from_left_ref[...], left)

    @pl.when(side == 1)
    def _():
        right = one_hot_columns(edge_ref[1:2, :], columns - width)
        out_ref[...] = inner_ref[...] + dot_last(from_right_ref[...], right)


def exchange(parts):
    count = len(parts)
    moved = [None] * count
    moved[0] = parts[0]
    for step in range(count - 1, 0, -1):
        moved[step] = lax.ppermute(parts[step], "conv", [(i, i ^ step) for i in range(count)])
    return moved


def to_right(value):
    count = lax.axis_size(("tile", "conv"))
    return lax.ppermute(value, ("tile", "conv"), [(i, (i + 1) % count) for i in range(count)])


def to_left(value):
    count = lax.axis_size(("tile", "conv"))
    return lax.ppermute(value, ("tile", "conv"), [((i + 1) % count, i) for i in range(count)])


def shape(dims, dtype):
    return jax.ShapeDtypeStruct(dims, dtype)


def on_device(field, interp, conv_blocks, band_shift, owner, edge_index):
    rows, columns = field.shape
    rim = edge_index.shape[1]
    points = owner.shape[0]
    groups = lax.axis_size("conv")
    blocks, _, block_points, _ = conv_blocks.shape
    slots = blocks * block_points
    capacity = slots // groups
    me = lax.axis_index("conv").astype(jnp.int32).reshape(1)
    owner_row = owner.reshape(1, points)

    whole = lambda dims: pl.BlockSpec(dims, lambda i: (0,) * len(dims))
    last = columns // rim - 1
    left_rim, right_rim = pl.pallas_call(
        functools.partial(rims_kernel, columns),
        grid=(1,),
        in_specs=[
            pl.BlockSpec((rows, rim), lambda i: (0, 0)),
            pl.BlockSpec((rows, rim), lambda i: (0, last)),
            whole(edge_index.shape),
        ],
        out_specs=[whole((rows, rim))] * 2,
        out_shape=[shape((rows, rim), BF16)] * 2,
        name="rims",
    )(field, field, edge_index)
    from_left = to_right(right_rim)
    from_right = to_left(left_rim)

    middle, place = pl.pallas_call(
        functools.partial(interior_kernel, groups, capacity),
        in_specs=[SMEM, VMEM, VMEM, VMEM],
        out_specs=[VMEM, VMEM],
        out_shape=[shape((rows, points), F32), shape((slots, points), BF16)],
        name="interior",
    )(me, field, interp, owner_row)

    packed = pl.pallas_call(
        functools.partial(subgrid_kernel, groups),
        in_specs=[VMEM] * 5,
        out_specs=[VMEM] * groups,
        out_shape=[shape((rows, capacity), BF16)] * groups,
        name="subgrid",
    )(middle, from_left, from_right, interp, place)

    adjoint = pl.pallas_call(
        functools.partial(convolve_kernel, groups),
        in_specs=[SMEM, SMEM] + [VMEM] * (groups + 1),
        out_specs=[VMEM] * groups,
        out_shape=[shape((rows, capacity), BF16)] * groups,
        scratch_shapes=[
            pltpu.VMEM((groups, rows, capacity), BF16),
            pltpu.VMEM((blocks, rows, block_points), BF16),
            pltpu.VMEM((blocks, rows, block_points), F32),
        ],
        name="convolve",
    )(me, band_shift, *exchange(packed), conv_blocks)

    returned, left_part, right_part = pl.pallas_call(
        functools.partial(edge_partial_kernel, groups, rim),
        in_specs=[VMEM] * (groups + 2),
        out_specs=[VMEM] * 3,
        out_shape=[shape((rows, points), BF16)] + [shape((rows, rim), BF16)] * 2,
        name="edge_partial",
    )(*exchange(adjoint), place, interp)
    left_sum = to_right(right_part)
    right_sum = to_left(left_part)

    inner = pl.pallas_call(
        functools.partial(interior_partial_kernel, rim),
        in_specs=[VMEM, VMEM],
        out_specs=VMEM,
        out_shape=shape((rows, columns), F32),
        name="interior_partial",
    )(returned, interp)

    edge_block = pl.BlockSpec((rows, rim), lambda i: (0, i * last))
    return pl.pallas_call(
        functools.partial(add_edges_kernel, columns),
        grid=(2,),
        in_specs=[whole((rows, rim)), whole((rows, rim)), whole(edge_index.shape), edge_block],
        out_specs=edge_block,
        out_shape=shape((rows, columns), F32),
        input_output_aliases={3: 0},
        name="add_edges",
    )(left_sum, right_sum, edge_index, inner)


def solution(mesh):
    return jax.shard_map(
        on_device,
        mesh=mesh,
        in_specs=(
            P(None, ("tile", "conv")),
            P(("tile", "conv"), None),
            P(("tile", "conv"), None, None, None),
            P(("tile", "conv"), None),
            P(("tile", "conv"), None),
            P(("tile", "conv"), None),
        ),
        out_specs=P(None, ("tile", "conv")),
        check_vma=False,
    )
```

```python
import functools

import jax
import jax.numpy as jnp
from jax import lax
from jax.experimental import pallas as pl
from jax.experimental.pallas import tpu as pltpu
from jax.sharding import PartitionSpec as P


F32 = jnp.float32
BF16 = jnp.bfloat16
VMEM = pl.BlockSpec(memory_space=pltpu.VMEM)
HBM = pl.BlockSpec(memory_space=pltpu.HBM)
SMEM = pl.BlockSpec(memory_space=pltpu.SMEM)


def dot(a, b):
    return jnp.dot(a, b, preferred_element_type=F32)


def dot_last(a, b):
    return lax.dot_general(a, b, (((1,), (1,)), ((), ())), preferred_element_type=F32)


def one_hot_columns(edge_row, offset):
    width = edge_row.shape[1]
    column = lax.broadcasted_iota(jnp.int32, (width, width), 0)
    return (column + offset == edge_row).astype(F32).astype(BF16)


def rims_kernel(columns, head_ref, tail_ref, edge_ref, left_ref, right_ref):
    width = edge_ref.shape[1]
    left = one_hot_columns(edge_ref[0:1, :], 0)
    right = one_hot_columns(edge_ref[1:2, :], columns - width)
    left_ref[...] = dot(head_ref[...].astype(BF16), left).astype(BF16)
    right_ref[...] = dot(tail_ref[...].astype(BF16), right).astype(BF16)


def interior_kernel(
    groups, capacity, me_ref, field_ref, interp_ref, owner_ref, conv_ref, edge_ref, mid_ref, place_ref
):
    del conv_ref, edge_ref
    columns = field_ref.shape[1]
    rim = (interp_ref.shape[0] - columns) // 2
    points = owner_ref.shape[1]
    mid_ref[...] = dot(field_ref[...].astype(BF16), interp_ref[rim : rim + columns, :])
    owners = owner_ref[...]
    group = lax.broadcasted_iota(jnp.int32, (max(groups, 16), points), 0)
    choose = (group == owners).astype(F32)
    earlier = lax.broadcasted_iota(jnp.int32, (points, points), 0) < lax.broadcasted_iota(
        jnp.int32, (points, points), 1
    )
    before = dot(choose.astype(BF16), earlier.astype(F32).astype(BF16))
    rank = jnp.sum(before * choose, axis=0, keepdims=True).astype(jnp.int32)
    slot = jnp.bitwise_xor(owners, me_ref[0]) * capacity + rank
    slots = lax.broadcasted_iota(jnp.int32, (groups * capacity, points), 0)
    place_ref[...] = (slots == slot).astype(F32).astype(BF16)


def subgrid_kernel(groups, mid_ref, from_left_ref, from_right_ref, interp_ref, place_ref, *outs):
    rim = from_left_ref.shape[1]
    high = interp_ref.shape[0] - rim
    subgrid = mid_ref[...] + dot(from_left_ref[...], interp_ref[:rim, :])
    subgrid = (subgrid + dot(from_right_ref[...], interp_ref[high:, :])).astype(BF16)
    packed = dot_last(subgrid, place_ref[...]).astype(BF16)
    capacity = packed.shape[1] // groups
    for step in range(groups):
        outs[step][...] = packed[:, step * capacity : (step + 1) * capacity]


def convolve_kernel(groups, me_ref, shift_ref, *refs):
    inputs = refs[:groups]
    conv_ref = refs[groups]
    outs = refs[groups + 1 : 2 * groups + 1]
    bands_ref, gathered_ref, adjoint_ref = refs[2 * groups + 1 :]
    me = me_ref[0]
    blocks, bands, points = conv_ref.shape[0], conv_ref.shape[1], conv_ref.shape[2]
    capacity = inputs[0].shape[1]
    per = points // capacity
    for step in range(groups):
        bands_ref[step] = inputs[step][...]
    for domain in range(groups):
        at = (domain % per) * capacity
        gathered_ref[domain // per, :, at : at + capacity] = bands_ref[jnp.bitwise_xor(me, domain)]
    adjoint_ref[...] = jnp.zeros_like(adjoint_ref)
    for j in range(blocks):
        source = [lax.rem(j + shift_ref[j, c], blocks) for c in range(bands)]
        forward = dot(gathered_ref[source[0]], conv_ref[j, 0])
        for c in range(1, bands):
            forward = forward + dot(gathered_ref[source[c]], conv_ref[j, c])
        forward = forward.astype(BF16)
        for c in range(bands):
            adjoint_ref[source[c]] += dot_last(forward, conv_ref[j, c])
    for domain in range(groups):
        at = (domain % per) * capacity
        bands_ref[domain] = adjoint_ref[domain // per, :, at : at + capacity].astype(BF16)
    for step in range(groups):
        outs[step][...] = bands_ref[jnp.bitwise_xor(me, step)]


def edge_partial_kernel(groups, rim, *refs):
    inputs = refs[:groups]
    place_ref, interp_ref, returned_ref, left_ref, right_ref = refs[groups:]
    packed = jnp.concatenate([ref[...] for ref in inputs], axis=1)
    returned = dot(packed, place_ref[...]).astype(BF16)
    returned_ref[...] = returned
    high = interp_ref.shape[0] - rim
    left_ref[...] = dot_last(returned, interp_ref[:rim, :]).astype(BF16)
    right_ref[...] = dot_last(returned, interp_ref[high:, :]).astype(BF16)


def interior_partial_kernel(rim, returned_ref, interp_ref, out_ref, rims_ref, middle, sem):
    high = interp_ref.shape[0] - rim
    inner_columns = middle.shape[1]
    returned = returned_ref[...]
    middle[...] = dot_last(returned, interp_ref[2 * rim : high - rim, :])
    copy = pltpu.make_async_copy(middle, out_ref.at[:, rim : rim + inner_columns], sem)
    copy.start()
    rims_ref[0] = dot_last(returned, interp_ref[rim : 2 * rim, :])
    rims_ref[1] = dot_last(returned, interp_ref[high - rim : high, :])
    copy.wait()


def add_edges_kernel(from_left_ref, from_right_ref, edge_ref, rims_ref, inner_ref, out_ref, sums, sems):
    del inner_ref
    rim = edge_ref.shape[1]
    columns = out_ref.shape[1]
    starts = (0, columns - rim)
    copies = []
    for side, received in enumerate((from_left_ref, from_right_ref)):
        chosen = one_hot_columns(edge_ref[side : side + 1, :], starts[side])
        sums[side] = rims_ref[side] + dot_last(received[...], chosen)
        at = starts[side]
        copy = pltpu.make_async_copy(sums.at[side], out_ref.at[:, at : at + rim], sems.at[side])
        copy.start()
        copies.append(copy)
    for copy in copies:
        copy.wait()


def near(value):
    return pltpu.with_memory_space_constraint(value, pltpu.VMEM)


def exchange(parts):
    count = len(parts)
    moved = [None] * count
    moved[0] = parts[0]
    for step in range(count - 1, 0, -1):
        moved[step] = lax.ppermute(parts[step], "conv", [(i, i ^ step) for i in range(count)])
    return moved


def to_right(value):
    count = lax.axis_size(("tile", "conv"))
    return lax.ppermute(value, ("tile", "conv"), [(i, (i + 1) % count) for i in range(count)])


def to_left(value):
    count = lax.axis_size(("tile", "conv"))
    return lax.ppermute(value, ("tile", "conv"), [((i + 1) % count, i) for i in range(count)])


def shape(dims, dtype):
    return jax.ShapeDtypeStruct(dims, dtype)


def on_device(field, interp, conv_blocks, band_shift, owner, edge_index):
    rows, columns = field.shape
    rim = edge_index.shape[1]
    points = owner.shape[0]
    groups = lax.axis_size("conv")
    blocks, _, block_points, _ = conv_blocks.shape
    slots = blocks * block_points
    capacity = slots // groups
    me = lax.axis_index("conv").astype(jnp.int32).reshape(1)
    owner_row = owner.reshape(1, points)

    whole = lambda dims: pl.BlockSpec(dims, lambda i: (0,) * len(dims))
    last = columns // rim - 1
    left_rim, right_rim = pl.pallas_call(
        functools.partial(rims_kernel, columns),
        grid=(1,),
        in_specs=[
            pl.BlockSpec((rows, rim), lambda i: (0, 0)),
            pl.BlockSpec((rows, rim), lambda i: (0, last)),
            whole(edge_index.shape),
        ],
        out_specs=[whole((rows, rim))] * 2,
        out_shape=[pltpu.VMEM((rows, rim), BF16)] * 2,
        name="rims",
    )(field, field, edge_index)
    from_left = to_right(right_rim)
    from_right = to_left(left_rim)

    interp, conv_blocks, edge_index = near(interp), near(conv_blocks), near(edge_index)
    middle, place = pl.pallas_call(
        functools.partial(interior_kernel, groups, capacity),
        in_specs=[SMEM] + [VMEM] * 5,
        out_specs=[VMEM, VMEM],
        out_shape=[pltpu.VMEM((rows, points), F32), pltpu.VMEM((slots, points), BF16)],
        name="interior",
    )(me, near(field), interp, owner_row, conv_blocks, edge_index)

    packed = pl.pallas_call(
        functools.partial(subgrid_kernel, groups),
        in_specs=[VMEM] * 5,
        out_specs=[VMEM] * groups,
        out_shape=[pltpu.VMEM((rows, capacity), BF16)] * groups,
        name="subgrid",
    )(near(middle), near(from_left), near(from_right), interp, near(place))

    adjoint = pl.pallas_call(
        functools.partial(convolve_kernel, groups),
        in_specs=[SMEM, SMEM] + [VMEM] * (groups + 1),
        out_specs=[VMEM] * groups,
        out_shape=[pltpu.VMEM((rows, capacity), BF16)] * groups,
        scratch_shapes=[
            pltpu.VMEM((groups, rows, capacity), BF16),
            pltpu.VMEM((blocks, rows, block_points), BF16),
            pltpu.VMEM((blocks, rows, block_points), F32),
        ],
        name="convolve",
    )(me, band_shift, *map(near, exchange(packed)), conv_blocks)

    returned, left_part, right_part = pl.pallas_call(
        functools.partial(edge_partial_kernel, groups, rim),
        in_specs=[VMEM] * (groups + 2),
        out_specs=[VMEM] * 3,
        out_shape=[pltpu.VMEM((rows, points), BF16)] + [pltpu.VMEM((rows, rim), BF16)] * 2,
        name="edge_partial",
    )(*map(near, exchange(adjoint)), near(place), interp)
    left_sum = to_right(right_part)
    right_sum = to_left(left_part)

    inner, rims = pl.pallas_call(
        functools.partial(interior_partial_kernel, rim),
        in_specs=[VMEM, VMEM],
        out_specs=[HBM, VMEM],
        out_shape=[shape((rows, columns), F32), pltpu.VMEM((2, rows, rim), F32)],
        scratch_shapes=[pltpu.VMEM((rows, columns - 2 * rim), F32), pltpu.SemaphoreType.DMA],
        name="interior_partial",
    )(near(returned), interp)

    return pl.pallas_call(
        add_edges_kernel,
        in_specs=[VMEM] * 4 + [HBM],
        out_specs=HBM,
        out_shape=shape((rows, columns), F32),
        scratch_shapes=[pltpu.VMEM((2, rows, rim), F32), pltpu.SemaphoreType.DMA((2,))],
        input_output_aliases={4: 0},
        name="add_edges",
    )(near(left_sum), near(right_sum), edge_index, near(rims), inner)


def solution(mesh):
    return jax.shard_map(
        on_device,
        mesh=mesh,
        in_specs=(
            P(None, ("tile", "conv")),
            P(("tile", "conv"), None),
            P(("tile", "conv"), None, None, None),
            P(("tile", "conv"), None),
            P(("tile", "conv"), None),
            P(("tile", "conv"), None),
        ),
        out_specs=P(None, ("tile", "conv")),
        check_vma=False,
    )
```

```python
import functools

import jax
import jax.numpy as jnp
from jax import lax
from jax.experimental import pallas as pl
from jax.experimental.pallas import tpu as pltpu
from jax.sharding import PartitionSpec as P


F32 = jnp.float32
BF16 = jnp.bfloat16
VMEM = pl.BlockSpec(memory_space=pltpu.VMEM)
HBM = pl.BlockSpec(memory_space=pltpu.HBM)
SMEM = pl.BlockSpec(memory_space=pltpu.SMEM)
PARAMS = pltpu.CompilerParams(vmem_limit_bytes=16 << 20)


def dot(a, b):
    return jnp.dot(a, b, preferred_element_type=F32)


def dot_last(a, b):
    return lax.dot_general(a, b, (((1,), (1,)), ((), ())), preferred_element_type=F32)


def one_hot_columns(edge_row, offset):
    width = edge_row.shape[1]
    column = lax.broadcasted_iota(jnp.int32, (width, width), 0)
    return (column + offset == edge_row).astype(F32).astype(BF16)


def rims_kernel(columns, head_ref, tail_ref, edge_ref, left_ref, right_ref):
    width = edge_ref.shape[1]
    left = one_hot_columns(edge_ref[0:1, :], 0)
    right = one_hot_columns(edge_ref[1:2, :], columns - width)
    left_ref[...] = dot(head_ref[...].astype(BF16), left).astype(BF16)
    right_ref[...] = dot(tail_ref[...].astype(BF16), right).astype(BF16)


def interior_kernel(
    groups,
    capacity,
    me_ref,
    field_ref,
    interp_ref,
    owner_ref,
    mid_ref,
    placed_ref,
):
    me = me_ref[0]
    columns = field_ref.shape[1]
    rim = (interp_ref.shape[0] - columns) // 2
    points = owner_ref.shape[1]
    owners = owner_ref[...]
    group = lax.broadcasted_iota(jnp.int32, (max(groups, 16), points), 0)
    choose = (group == owners).astype(F32)
    earlier = lax.broadcasted_iota(jnp.int32, (points, points), 0) < lax.broadcasted_iota(
        jnp.int32, (points, points), 1
    )
    before = dot(choose.astype(BF16), earlier.astype(F32).astype(BF16))
    rank = jnp.sum(before * choose, axis=0, keepdims=True).astype(jnp.int32)
    slot = jnp.bitwise_xor(owners, me) * capacity + rank
    slots = lax.broadcasted_iota(jnp.int32, (groups * capacity, points), 0)
    place = (slots == slot).astype(F32).astype(BF16)
    placed_ref[...] = dot_last(interp_ref[...], place).astype(BF16)
    mid_ref[...] = dot(field_ref[...].astype(BF16), placed_ref[rim : rim + columns, :])


def matrix_kernel(groups, capacity, me_ref, shift_ref, conv_ref, edge_ref, after_ref, matrix_ref, in_order):
    del edge_ref, after_ref
    me = me_ref[0]
    blocks, bands, size = conv_ref.shape[0], conv_ref.shape[1], conv_ref.shape[2]
    for j in range(blocks):
        source = [lax.rem(j + shift_ref[j, c], blocks) for c in range(bands)]
        weights = [conv_ref[j, c].astype(F32) for c in range(bands)]
        for s in range(blocks):
            total = jnp.where(source[0] == s, weights[0], 0.0)
            for c in range(1, bands):
                total = total + jnp.where(source[c] == s, weights[c], 0.0)
            in_order[s * size : (s + 1) * size, j * size : (j + 1) * size] = total.astype(BF16)
    for step in range(groups):
        at = pl.multiple_of(jnp.bitwise_xor(me, step) * capacity, capacity)
        matrix_ref[step * capacity : (step + 1) * capacity, :] = in_order[pl.ds(at, capacity), :]


def split(value, outs):
    capacity = value.shape[1] // len(outs)
    for step, out in enumerate(outs):
        out[...] = value[:, step * capacity : (step + 1) * capacity]


def joined(refs):
    return jnp.concatenate([ref[...] for ref in refs], axis=1)


def subgrid_kernel(mid_ref, from_left_ref, from_right_ref, placed_ref, *outs):
    rim = from_left_ref.shape[1]
    high = placed_ref.shape[0] - rim
    packed = mid_ref[...] + dot(from_left_ref[...], placed_ref[:rim, :])
    packed = packed + dot(from_right_ref[...], placed_ref[high:, :])
    split(packed.astype(BF16), outs)


def convolve_kernel(groups, *refs):
    inputs, matrix_ref, outs = refs[:groups], refs[groups], refs[groups + 1 :]
    forward = dot(joined(inputs), matrix_ref[...]).astype(BF16)
    split(dot_last(forward, matrix_ref[...]).astype(BF16), outs)


def edge_partial_kernel(groups, rim, *refs):
    inputs = refs[:groups]
    placed_ref, returned_ref, left_ref, right_ref = refs[groups:]
    returned = joined(inputs)
    high = placed_ref.shape[0] - rim
    right_ref[...] = dot_last(returned, placed_ref[high:, :]).astype(BF16)
    left_ref[...] = dot_last(returned, placed_ref[:rim, :]).astype(BF16)
    returned_ref[...] = returned


def interior_partial_kernel(rim, returned_ref, placed_ref, out_ref, rims_ref, middle, sem):
    high = placed_ref.shape[0] - rim
    inner_columns = middle.shape[1]
    returned = returned_ref[...]
    middle[...] = dot_last(returned, placed_ref[2 * rim : high - rim, :])
    copy = pltpu.make_async_copy(middle, out_ref.at[:, rim : rim + inner_columns], sem)
    copy.start()
    rims_ref[0] = dot_last(returned, placed_ref[rim : 2 * rim, :])
    rims_ref[1] = dot_last(returned, placed_ref[high - rim : high, :])
    copy.wait()


def add_edges_kernel(side, received_ref, edge_ref, rims_ref, inner_ref, out_ref, sums, sem):
    del inner_ref
    rim = edge_ref.shape[1]
    at = (out_ref.shape[1] - rim) * side
    chosen = one_hot_columns(edge_ref[side : side + 1, :], at)
    sums[...] = rims_ref[side] + dot_last(received_ref[...], chosen)
    copy = pltpu.make_async_copy(sums, out_ref.at[:, at : at + rim], sem)
    copy.start()
    copy.wait()


def far(value):
    return pltpu.with_memory_space_constraint(value, pltpu.HBM)


def near(value):
    return pltpu.with_memory_space_constraint(value, pltpu.VMEM)


def exchange(parts):
    count = len(parts)
    moved = [None] * count
    moved[0] = parts[0]
    for step in range(1, count):
        moved[step] = lax.ppermute(parts[step], "conv", [(i, i ^ step) for i in range(count)])
    return moved


def to_right(value):
    count = lax.axis_size(("tile", "conv"))
    return lax.ppermute(value, ("tile", "conv"), [(i, (i + 1) % count) for i in range(count)])


def to_left(value):
    count = lax.axis_size(("tile", "conv"))
    return lax.ppermute(value, ("tile", "conv"), [((i + 1) % count, i) for i in range(count)])


def shape(dims, dtype):
    return jax.ShapeDtypeStruct(dims, dtype)


def on_device(field, interp, conv_blocks, band_shift, owner, edge_index):
    rows, columns = field.shape
    rim = edge_index.shape[1]
    points = owner.shape[0]
    groups = lax.axis_size("conv")
    blocks, _, block_points, _ = conv_blocks.shape
    slots = blocks * block_points
    capacity = slots // groups
    me = lax.axis_index("conv").astype(jnp.int32).reshape(1)
    owner_row = owner.reshape(1, points)

    whole = lambda dims: pl.BlockSpec(dims, lambda i: (0,) * len(dims))
    last = columns // rim - 1
    left_rim, right_rim = pl.pallas_call(
        functools.partial(rims_kernel, columns),
        grid=(1,),
        in_specs=[
            pl.BlockSpec((rows, rim), lambda i: (0, 0)),
            pl.BlockSpec((rows, rim), lambda i: (0, last)),
            whole(edge_index.shape),
        ],
        out_specs=[whole((rows, rim))] * 2,
        out_shape=[pltpu.VMEM((rows, rim), BF16)] * 2,
        compiler_params=PARAMS,
        name="rims",
    )(far(field), far(field), far(edge_index))
    from_left = to_right(right_rim)
    from_right = to_left(left_rim)

    interp, conv_blocks, edge_index = near(interp), near(conv_blocks), near(edge_index)
    middle, placed = pl.pallas_call(
        functools.partial(interior_kernel, groups, capacity),
        in_specs=[SMEM] + [VMEM] * 3,
        out_specs=[VMEM] * 2,
        out_shape=[
            pltpu.VMEM((rows, slots), F32),
            pltpu.VMEM((interp.shape[0], slots), BF16),
        ],
        compiler_params=PARAMS,
        name="interior",
    )(me, near(field), interp, owner_row)
    placed = near(placed)

    packed = pl.pallas_call(
        subgrid_kernel,
        in_specs=[VMEM] * 4,
        out_specs=[VMEM] * groups,
        out_shape=[pltpu.VMEM((rows, capacity), BF16)] * groups,
        compiler_params=PARAMS,
        name="subgrid",
    )(near(middle), near(from_left), near(from_right), placed)

    matrix = pl.pallas_call(
        functools.partial(matrix_kernel, groups, capacity),
        in_specs=[SMEM, SMEM] + [VMEM] * 3,
        out_specs=VMEM,
        out_shape=pltpu.VMEM((slots, slots), BF16),
        scratch_shapes=[pltpu.VMEM((slots, slots), BF16)],
        compiler_params=PARAMS,
        name="matrix",
    )(me, band_shift, conv_blocks, edge_index, near(packed[0]))

    adjoint = pl.pallas_call(
        functools.partial(convolve_kernel, groups),
        in_specs=[VMEM] * (groups + 1),
        out_specs=[VMEM] * groups,
        out_shape=[pltpu.VMEM((rows, capacity), BF16)] * groups,
        compiler_params=PARAMS,
        name="convolve",
    )(*map(near, exchange(packed)), near(matrix))

    returned, left_part, right_part = pl.pallas_call(
        functools.partial(edge_partial_kernel, groups, rim),
        in_specs=[VMEM] * (groups + 1),
        out_specs=[VMEM] * 3,
        out_shape=[pltpu.VMEM((rows, slots), BF16)] + [pltpu.VMEM((rows, rim), BF16)] * 2,
        compiler_params=PARAMS,
        name="edge_partial",
    )(*map(near, exchange(adjoint)), placed)
    sums = (to_right(right_part), to_left(left_part))

    result, rims = pl.pallas_call(
        functools.partial(interior_partial_kernel, rim),
        in_specs=[VMEM, VMEM],
        out_specs=[HBM, VMEM],
        out_shape=[shape((rows, columns), F32), pltpu.VMEM((2, rows, rim), F32)],
        scratch_shapes=[pltpu.VMEM((rows, columns - 2 * rim), F32), pltpu.SemaphoreType.DMA],
        compiler_params=PARAMS,
        name="interior_partial",
    )(near(returned), placed)

    for side in range(2):
        result = pl.pallas_call(
            functools.partial(add_edges_kernel, side),
            in_specs=[VMEM] * 3 + [HBM],
            out_specs=HBM,
            out_shape=shape((rows, columns), F32),
            scratch_shapes=[pltpu.VMEM((rows, rim), F32), pltpu.SemaphoreType.DMA],
            input_output_aliases={3: 0},
            compiler_params=PARAMS,
            name=f"add_edges_{side}",
        )(near(sums[side]), edge_index, near(rims), result)
    return result


def solution(mesh):
    return jax.shard_map(
        on_device,
        mesh=mesh,
        in_specs=(
            P(None, ("tile", "conv")),
            P(("tile", "conv"), None),
            P(("tile", "conv"), None, None, None),
            P(("tile", "conv"), None),
            P(("tile", "conv"), None),
            P(("tile", "conv"), None),
        ),
        out_specs=P(None, ("tile", "conv")),
        check_vma=False,
    )
```

```python
import functools

import jax
import jax.numpy as jnp
from jax import lax
from jax.experimental import pallas as pl
from jax.experimental.pallas import tpu as pltpu
from jax.sharding import PartitionSpec as P


F32 = jnp.float32
BF16 = jnp.bfloat16
VMEM = pl.BlockSpec(memory_space=pltpu.VMEM)
HBM = pl.BlockSpec(memory_space=pltpu.HBM)
SMEM = pl.BlockSpec(memory_space=pltpu.SMEM)
PARAMS = pltpu.CompilerParams(vmem_limit_bytes=16 << 20)


def dot(a, b):
    return jnp.dot(a, b, preferred_element_type=F32)


def dot_last(a, b):
    return lax.dot_general(a, b, (((1,), (1,)), ((), ())), preferred_element_type=F32)


def one_hot_columns(edge_row, offset):
    width = edge_row.shape[1]
    column = lax.broadcasted_iota(jnp.int32, (width, width), 0)
    return (column + offset == edge_row).astype(F32).astype(BF16)


def rims_kernel(field_ref, edge_ref, left_ref, right_ref, ends, lists, sems):
    width = edge_ref.shape[1]
    starts = (0, field_ref.shape[1] - width)
    copies = [pltpu.make_async_copy(edge_ref, lists, sems.at[2])]
    for side, at in enumerate(starts):
        source = field_ref.at[:, at : at + width]
        copies.append(pltpu.make_async_copy(source, ends.at[side], sems.at[side]))
    for copy in copies:
        copy.start()
    copies[0].wait()
    chosen = [one_hot_columns(lists[side : side + 1, :], at) for side, at in enumerate(starts)]
    for side, out in enumerate((left_ref, right_ref)):
        copies[1 + side].wait()
        out[...] = dot(ends[side].astype(BF16), chosen[side]).astype(BF16)


def interior_kernel(
    groups,
    capacity,
    me_ref,
    field_ref,
    interp_ref,
    owner_ref,
    mid_ref,
    placed_ref,
):
    me = me_ref[0]
    columns = field_ref.shape[1]
    rim = (interp_ref.shape[0] - columns) // 2
    points = owner_ref.shape[1]
    owners = owner_ref[...]
    group = lax.broadcasted_iota(jnp.int32, (max(groups, 16), points), 0)
    choose = (group == owners).astype(F32)
    earlier = lax.broadcasted_iota(jnp.int32, (points, points), 0) < lax.broadcasted_iota(
        jnp.int32, (points, points), 1
    )
    before = dot(choose.astype(BF16), earlier.astype(F32).astype(BF16))
    rank = jnp.sum(before * choose, axis=0, keepdims=True).astype(jnp.int32)
    slot = jnp.bitwise_xor(owners, me) * capacity + rank
    slots = lax.broadcasted_iota(jnp.int32, (groups * capacity, points), 0)
    place = (slots == slot).astype(F32).astype(BF16)
    placed_ref[...] = dot_last(interp_ref[...], place).astype(BF16)
    mid_ref[...] = dot(field_ref[...].astype(BF16), placed_ref[rim : rim + columns, :])


def matrix_kernel(groups, capacity, me_ref, shift_ref, conv_ref, edge_ref, after_ref, matrix_ref, in_order):
    del edge_ref, after_ref
    me = me_ref[0]
    blocks, bands, size = conv_ref.shape[0], conv_ref.shape[1], conv_ref.shape[2]
    for j in range(blocks):
        source = [lax.rem(j + shift_ref[j, c], blocks) for c in range(bands)]
        weights = [conv_ref[j, c].astype(F32) for c in range(bands)]
        for s in range(blocks):
            total = jnp.where(source[0] == s, weights[0], 0.0)
            for c in range(1, bands):
                total = total + jnp.where(source[c] == s, weights[c], 0.0)
            in_order[s * size : (s + 1) * size, j * size : (j + 1) * size] = total.astype(BF16)
    for step in range(groups):
        at = pl.multiple_of(jnp.bitwise_xor(me, step) * capacity, capacity)
        matrix_ref[step * capacity : (step + 1) * capacity, :] = in_order[pl.ds(at, capacity), :]


def split(value, outs):
    capacity = value.shape[1] // len(outs)
    for step, out in enumerate(outs):
        out[...] = value[:, step * capacity : (step + 1) * capacity]


def joined(refs):
    return jnp.concatenate([ref[...] for ref in refs], axis=1)


def subgrid_kernel(mid_ref, from_left_ref, from_right_ref, placed_ref, *outs):
    rim = from_left_ref.shape[1]
    high = placed_ref.shape[0] - rim
    packed = mid_ref[...] + dot(from_left_ref[...], placed_ref[:rim, :])
    packed = packed + dot(from_right_ref[...], placed_ref[high:, :])
    split(packed.astype(BF16), outs)


def convolve_kernel(groups, *refs):
    inputs, matrix_ref, outs = refs[:groups], refs[groups], refs[groups + 1 :]
    forward = dot(joined(inputs), matrix_ref[...]).astype(BF16)
    split(dot_last(forward, matrix_ref[...]).astype(BF16), outs)


def edge_partial_kernel(groups, rim, *refs):
    inputs = refs[:groups]
    placed_ref, returned_ref, left_ref, right_ref = refs[groups:]
    returned = joined(inputs)
    high = placed_ref.shape[0] - rim
    right_ref[...] = dot_last(returned, placed_ref[high:, :]).astype(BF16)
    left_ref[...] = dot_last(returned, placed_ref[:rim, :]).astype(BF16)
    returned_ref[...] = returned


def interior_partial_kernel(rim, returned_ref, placed_ref, out_ref, rims_ref, middle, sem):
    high = placed_ref.shape[0] - rim
    inner_columns = middle.shape[1]
    returned = returned_ref[...]
    middle[...] = dot_last(returned, placed_ref[2 * rim : high - rim, :])
    copy = pltpu.make_async_copy(middle, out_ref.at[:, rim : rim + inner_columns], sem)
    copy.start()
    rims_ref[0] = dot_last(returned, placed_ref[rim : 2 * rim, :])
    rims_ref[1] = dot_last(returned, placed_ref[high - rim : high, :])
    copy.wait()


def add_edges_kernel(side, received_ref, edge_ref, rims_ref, inner_ref, out_ref, sums, sem):
    del inner_ref
    rim = edge_ref.shape[1]
    at = (out_ref.shape[1] - rim) * side
    chosen = one_hot_columns(edge_ref[side : side + 1, :], at)
    sums[...] = rims_ref[side] + dot_last(received_ref[...], chosen)
    copy = pltpu.make_async_copy(sums, out_ref.at[:, at : at + rim], sem)
    copy.start()
    copy.wait()


def far(value):
    return pltpu.with_memory_space_constraint(value, pltpu.HBM)


def near(value):
    return pltpu.with_memory_space_constraint(value, pltpu.VMEM)


def exchange(parts):
    count = len(parts)
    moved = [None] * count
    moved[0] = parts[0]
    for step in range(1, count):
        moved[step] = lax.ppermute(parts[step], "conv", [(i, i ^ step) for i in range(count)])
    return moved


def to_right(value):
    count = lax.axis_size(("tile", "conv"))
    return lax.ppermute(value, ("tile", "conv"), [(i, (i + 1) % count) for i in range(count)])


def to_left(value):
    count = lax.axis_size(("tile", "conv"))
    return lax.ppermute(value, ("tile", "conv"), [((i + 1) % count, i) for i in range(count)])


def shape(dims, dtype):
    return jax.ShapeDtypeStruct(dims, dtype)


def on_device(field, interp, conv_blocks, band_shift, owner, edge_index):
    rows, columns = field.shape
    rim = edge_index.shape[1]
    points = owner.shape[0]
    groups = lax.axis_size("conv")
    blocks, _, block_points, _ = conv_blocks.shape
    slots = blocks * block_points
    capacity = slots // groups
    me = lax.axis_index("conv").astype(jnp.int32).reshape(1)
    owner_row = owner.reshape(1, points)

    left_rim, right_rim = pl.pallas_call(
        rims_kernel,
        in_specs=[HBM, HBM],
        out_specs=[VMEM, VMEM],
        out_shape=[pltpu.VMEM((rows, rim), BF16)] * 2,
        scratch_shapes=[
            pltpu.VMEM((2, rows, rim), F32),
            pltpu.VMEM(edge_index.shape, jnp.int32),
            pltpu.SemaphoreType.DMA((3,)),
        ],
        compiler_params=PARAMS,
        name="rims",
    )(far(field), far(edge_index))
    from_left = to_right(right_rim)
    from_right = to_left(left_rim)

    interp, conv_blocks, edge_index = near(interp), near(conv_blocks), near(edge_index)
    middle, placed = pl.pallas_call(
        functools.partial(interior_kernel, groups, capacity),
        in_specs=[SMEM] + [VMEM] * 3,
        out_specs=[VMEM] * 2,
        out_shape=[
            pltpu.VMEM((rows, slots), F32),
            pltpu.VMEM((interp.shape[0], slots), BF16),
        ],
        compiler_params=PARAMS,
        name="interior",
    )(me, near(field), interp, owner_row)
    placed = near(placed)

    packed = pl.pallas_call(
        subgrid_kernel,
        in_specs=[VMEM] * 4,
        out_specs=[VMEM] * groups,
        out_shape=[pltpu.VMEM((rows, capacity), BF16)] * groups,
        compiler_params=PARAMS,
        name="subgrid",
    )(near(middle), near(from_left), near(from_right), placed)

    matrix = pl.pallas_call(
        functools.partial(matrix_kernel, groups, capacity),
        in_specs=[SMEM, SMEM] + [VMEM] * 3,
        out_specs=VMEM,
        out_shape=pltpu.VMEM((slots, slots), BF16),
        scratch_shapes=[pltpu.VMEM((slots, slots), BF16)],
        compiler_params=PARAMS,
        name="matrix",
    )(me, band_shift, conv_blocks, edge_index, near(packed[0]))

    adjoint = pl.pallas_call(
        functools.partial(convolve_kernel, groups),
        in_specs=[VMEM] * (groups + 1),
        out_specs=[VMEM] * groups,
        out_shape=[pltpu.VMEM((rows, capacity), BF16)] * groups,
        compiler_params=PARAMS,
        name="convolve",
    )(*map(near, exchange(packed)), near(matrix))

    returned, left_part, right_part = pl.pallas_call(
        functools.partial(edge_partial_kernel, groups, rim),
        in_specs=[VMEM] * (groups + 1),
        out_specs=[VMEM] * 3,
        out_shape=[pltpu.VMEM((rows, slots), BF16)] + [pltpu.VMEM((rows, rim), BF16)] * 2,
        compiler_params=PARAMS,
        name="edge_partial",
    )(*map(near, exchange(adjoint)), placed)
    sums = (to_right(right_part), to_left(left_part))

    result, rims = pl.pallas_call(
        functools.partial(interior_partial_kernel, rim),
        in_specs=[VMEM, VMEM],
        out_specs=[HBM, VMEM],
        out_shape=[shape((rows, columns), F32), pltpu.VMEM((2, rows, rim), F32)],
        scratch_shapes=[pltpu.VMEM((rows, columns - 2 * rim), F32), pltpu.SemaphoreType.DMA],
        compiler_params=PARAMS,
        name="interior_partial",
    )(near(returned), placed)

    for side in range(2):
        result = pl.pallas_call(
            functools.partial(add_edges_kernel, side),
            in_specs=[VMEM] * 3 + [HBM],
            out_specs=HBM,
            out_shape=shape((rows, columns), F32),
            scratch_shapes=[pltpu.VMEM((rows, rim), F32), pltpu.SemaphoreType.DMA],
            input_output_aliases={3: 0},
            compiler_params=PARAMS,
        )(near(sums[side]), edge_index, near(rims), result)
    return result


def solution(mesh):
    return jax.shard_map(
        on_device,
        mesh=mesh,
        in_specs=(
            P(None, ("tile", "conv")),
            P(("tile", "conv"), None),
            P(("tile", "conv"), None, None, None),
            P(("tile", "conv"), None),
            P(("tile", "conv"), None),
            P(("tile", "conv"), None),
        ),
        out_specs=P(None, ("tile", "conv")),
        check_vma=False,
    )
```

```python
import functools

import jax
import jax.numpy as jnp
from jax import lax
from jax.experimental import pallas as pl
from jax.experimental.pallas import tpu as pltpu
from jax.sharding import PartitionSpec as P


F32 = jnp.float32
BF16 = jnp.bfloat16
VMEM = pl.BlockSpec(memory_space=pltpu.VMEM)
HBM = pl.BlockSpec(memory_space=pltpu.HBM)
SMEM = pl.BlockSpec(memory_space=pltpu.SMEM)
PARAMS = pltpu.CompilerParams(vmem_limit_bytes=16 << 20)


def dot(a, b):
    return jnp.dot(a, b, preferred_element_type=F32)


def dot_last(a, b):
    return lax.dot_general(a, b, (((1,), (1,)), ((), ())), preferred_element_type=F32)


def one_hot_columns(edge_row, offset):
    width = edge_row.shape[1]
    column = lax.broadcasted_iota(jnp.int32, (width, width), 0)
    return (column + offset == edge_row).astype(F32).astype(BF16)


def rims_kernel(columns, me_ref, head_ref, tail_ref, edge_ref, far_ref, near_ref):
    width = edge_ref.shape[1]
    odd = lax.rem(me_ref[0], 2) == 1
    left = one_hot_columns(edge_ref[0:1, :], 0)
    right = one_hot_columns(edge_ref[1:2, :], columns - width)
    left = dot(head_ref[...].astype(BF16), left)
    right = dot(tail_ref[...].astype(BF16), right)
    far_ref[...] = jnp.where(odd, right, left).astype(BF16)
    near_ref[...] = jnp.where(odd, left, right).astype(BF16)


def interior_kernel(
    groups,
    capacity,
    me_ref,
    field_ref,
    interp_ref,
    owner_ref,
    mid_ref,
    placed_ref,
):
    me = me_ref[0]
    columns = field_ref.shape[1]
    rim = (interp_ref.shape[0] - columns) // 2
    points = owner_ref.shape[1]
    owners = owner_ref[...]
    group = lax.broadcasted_iota(jnp.int32, (max(groups, 16), points), 0)
    choose = (group == owners).astype(F32)
    earlier = lax.broadcasted_iota(jnp.int32, (points, points), 0) < lax.broadcasted_iota(
        jnp.int32, (points, points), 1
    )
    before = dot(choose.astype(BF16), earlier.astype(F32).astype(BF16))
    rank = jnp.sum(before * choose, axis=0, keepdims=True).astype(jnp.int32)
    slot = jnp.bitwise_xor(owners, me) * capacity + rank
    slots = lax.broadcasted_iota(jnp.int32, (groups * capacity, points), 0)
    place = (slots == slot).astype(F32).astype(BF16)
    placed_ref[...] = dot_last(interp_ref[...], place).astype(BF16)
    mid_ref[...] = dot(field_ref[...].astype(BF16), placed_ref[rim : rim + columns, :])


def matrix_kernel(groups, capacity, me_ref, shift_ref, conv_ref, edge_ref, after_ref, matrix_ref, in_order):
    del edge_ref, after_ref
    me = me_ref[0]
    blocks, bands, size = conv_ref.shape[0], conv_ref.shape[1], conv_ref.shape[2]
    for j in range(blocks):
        source = [lax.rem(j + shift_ref[j, c], blocks) for c in range(bands)]
        weights = [conv_ref[j, c].astype(F32) for c in range(bands)]
        for s in range(blocks):
            total = jnp.where(source[0] == s, weights[0], 0.0)
            for c in range(1, bands):
                total = total + jnp.where(source[c] == s, weights[c], 0.0)
            in_order[s * size : (s + 1) * size, j * size : (j + 1) * size] = total.astype(BF16)
    for step in range(groups):
        at = pl.multiple_of(jnp.bitwise_xor(me, step) * capacity, capacity)
        matrix_ref[step * capacity : (step + 1) * capacity, :] = in_order[pl.ds(at, capacity), :]


def split(value, outs):
    capacity = value.shape[1] // len(outs)
    for step, out in enumerate(outs):
        out[...] = value[:, step * capacity : (step + 1) * capacity]


def joined(refs):
    return jnp.concatenate([ref[...] for ref in refs], axis=1)


def rim_rows(me_ref, placed_ref, rim, towards_odd):
    at = (placed_ref.shape[0] - rim) * (lax.rem(me_ref[0], 2) == towards_odd).astype(jnp.int32)
    return placed_ref[pl.ds(pl.multiple_of(at, rim), rim), :]


def subgrid_kernel(me_ref, mid_ref, from_far_ref, from_near_ref, placed_ref, *outs):
    rim = from_far_ref.shape[1]
    packed = mid_ref[...] + dot(from_far_ref[...], rim_rows(me_ref, placed_ref, rim, 1))
    packed = packed + dot(from_near_ref[...], rim_rows(me_ref, placed_ref, rim, 0))
    split(packed.astype(BF16), outs)


def convolve_kernel(groups, *refs):
    inputs, matrix_ref, outs = refs[:groups], refs[groups], refs[groups + 1 :]
    forward = dot(joined(inputs), matrix_ref[...]).astype(BF16)
    split(dot_last(forward, matrix_ref[...]).astype(BF16), outs)


def edge_partial_kernel(groups, rim, me_ref, *refs):
    inputs = refs[:groups]
    placed_ref, returned_ref, far_ref, near_ref = refs[groups:]
    returned = joined(inputs)
    far_ref[...] = dot_last(returned, rim_rows(me_ref, placed_ref, rim, 1)).astype(BF16)
    near_ref[...] = dot_last(returned, rim_rows(me_ref, placed_ref, rim, 0)).astype(BF16)
    returned_ref[...] = returned


def interior_partial_kernel(rim, returned_ref, placed_ref, out_ref, rims_ref, middle, sem):
    high = placed_ref.shape[0] - rim
    inner_columns = middle.shape[1]
    returned = returned_ref[...]
    middle[...] = dot_last(returned, placed_ref[2 * rim : high - rim, :])
    copy = pltpu.make_async_copy(middle, out_ref.at[:, rim : rim + inner_columns], sem)
    copy.start()
    rims_ref[0] = dot_last(returned, placed_ref[rim : 2 * rim, :])
    rims_ref[1] = dot_last(returned, placed_ref[high - rim : high, :])
    copy.wait()


def add_edges_kernel(towards_odd, me_ref, received_ref, edge_ref, rims_ref, inner_ref, out_ref, sums, sem):
    del inner_ref
    rim = edge_ref.shape[1]
    side = (lax.rem(me_ref[0], 2) == towards_odd).astype(jnp.int32)
    at = pl.multiple_of((out_ref.shape[1] - rim) * side, rim)
    chosen = one_hot_columns(edge_ref[pl.ds(side, 1), :], at)
    sums[...] = rims_ref[side] + dot_last(received_ref[...], chosen)
    copy = pltpu.make_async_copy(sums, out_ref.at[:, pl.ds(at, rim)], sem)
    copy.start()
    copy.wait()


def far(value):
    return pltpu.with_memory_space_constraint(value, pltpu.HBM)


def near(value):
    return pltpu.with_memory_space_constraint(value, pltpu.VMEM)


def exchange(parts):
    count = len(parts)
    moved = [None] * count
    moved[0] = parts[0]
    for step in range(1, count):
        moved[step] = lax.ppermute(parts[step], "conv", [(i, i ^ step) for i in range(count)])
    return moved


def swap(value, first):
    count = lax.axis_size(("tile", "conv"))
    pairs = [(i, (i + 1) % count) for i in range(first, count, 2)]
    return lax.ppermute(value, ("tile", "conv"), pairs + [(j, i) for i, j in pairs])


def shape(dims, dtype):
    return jax.ShapeDtypeStruct(dims, dtype)


def on_device(field, interp, conv_blocks, band_shift, owner, edge_index):
    rows, columns = field.shape
    rim = edge_index.shape[1]
    points = owner.shape[0]
    groups = lax.axis_size("conv")
    blocks, _, block_points, _ = conv_blocks.shape
    slots = blocks * block_points
    capacity = slots // groups
    me = lax.axis_index("conv").astype(jnp.int32).reshape(1)
    owner_row = owner.reshape(1, points)

    whole = lambda dims: pl.BlockSpec(dims, lambda i: (0,) * len(dims))
    last = columns // rim - 1
    far_rim, near_rim = pl.pallas_call(
        functools.partial(rims_kernel, columns),
        grid=(1,),
        in_specs=[
            SMEM,
            pl.BlockSpec((rows, rim), lambda i: (0, 0)),
            pl.BlockSpec((rows, rim), lambda i: (0, last)),
            whole(edge_index.shape),
        ],
        out_specs=[whole((rows, rim))] * 2,
        out_shape=[pltpu.VMEM((rows, rim), BF16)] * 2,
        compiler_params=PARAMS,
        name="rims",
    )(me, far(field), far(field), far(edge_index))
    from_far = swap(far_rim, 1)
    from_near = swap(near_rim, 0)

    interp, conv_blocks, edge_index = near(interp), near(conv_blocks), near(edge_index)
    middle, placed = pl.pallas_call(
        functools.partial(interior_kernel, groups, capacity),
        in_specs=[SMEM] + [VMEM] * 3,
        out_specs=[VMEM] * 2,
        out_shape=[
            pltpu.VMEM((rows, slots), F32),
            pltpu.VMEM((interp.shape[0], slots), BF16),
        ],
        compiler_params=PARAMS,
        name="interior",
    )(me, near(field), interp, owner_row)
    placed = near(placed)

    packed = pl.pallas_call(
        subgrid_kernel,
        in_specs=[SMEM] + [VMEM] * 4,
        out_specs=[VMEM] * groups,
        out_shape=[pltpu.VMEM((rows, capacity), BF16)] * groups,
        compiler_params=PARAMS,
        name="subgrid",
    )(me, near(middle), near(from_far), near(from_near), placed)

    matrix = pl.pallas_call(
        functools.partial(matrix_kernel, groups, capacity),
        in_specs=[SMEM, SMEM] + [VMEM] * 3,
        out_specs=VMEM,
        out_shape=pltpu.VMEM((slots, slots), BF16),
        scratch_shapes=[pltpu.VMEM((slots, slots), BF16)],
        compiler_params=PARAMS,
        name="matrix",
    )(me, band_shift, conv_blocks, edge_index, near(packed[0]))

    adjoint = pl.pallas_call(
        functools.partial(convolve_kernel, groups),
        in_specs=[VMEM] * (groups + 1),
        out_specs=[VMEM] * groups,
        out_shape=[pltpu.VMEM((rows, capacity), BF16)] * groups,
        compiler_params=PARAMS,
        name="convolve",
    )(*map(near, exchange(packed)), near(matrix))

    returned, far_part, near_part = pl.pallas_call(
        functools.partial(edge_partial_kernel, groups, rim),
        in_specs=[SMEM] + [VMEM] * (groups + 1),
        out_specs=[VMEM] * 3,
        out_shape=[pltpu.VMEM((rows, slots), BF16)] + [pltpu.VMEM((rows, rim), BF16)] * 2,
        compiler_params=PARAMS,
        name="edge_partial",
    )(me, *map(near, exchange(adjoint)), placed)
    sums = ((0, swap(near_part, 0)), (1, swap(far_part, 1)))

    result, rims = pl.pallas_call(
        functools.partial(interior_partial_kernel, rim),
        in_specs=[VMEM, VMEM],
        out_specs=[HBM, VMEM],
        out_shape=[shape((rows, columns), F32), pltpu.VMEM((2, rows, rim), F32)],
        scratch_shapes=[pltpu.VMEM((rows, columns - 2 * rim), F32), pltpu.SemaphoreType.DMA],
        compiler_params=PARAMS,
        name="interior_partial",
    )(near(returned), placed)

    for towards_odd, received in sums:
        result = pl.pallas_call(
            functools.partial(add_edges_kernel, towards_odd),
            in_specs=[SMEM] + [VMEM] * 3 + [HBM],
            out_specs=HBM,
            out_shape=shape((rows, columns), F32),
            scratch_shapes=[pltpu.VMEM((rows, rim), F32), pltpu.SemaphoreType.DMA],
            input_output_aliases={4: 0},
            compiler_params=PARAMS,
        )(me, near(received), edge_index, near(rims), result)
    return result


def solution(mesh):
    return jax.shard_map(
        on_device,
        mesh=mesh,
        in_specs=(
            P(None, ("tile", "conv")),
            P(("tile", "conv"), None),
            P(("tile", "conv"), None, None, None),
            P(("tile", "conv"), None),
            P(("tile", "conv"), None),
            P(("tile", "conv"), None),
        ),
        out_specs=P(None, ("tile", "conv")),
        check_vma=False,
    )
```
